32 devices in a mesh: grp: 4 (over x, core), dp: 8 (over z, y).
Axes of the slice: x: 2, y: 2, z: 4, core: 2. Of those that a mesh axis runs over, the one named last changes fastest.
Arguments:
- gradients: bfloat16 [4, 8, 16384, 128], P('grp', 'dp'), may hold values from -48 to 48
- block_len: int32 [16], replicated, may hold values from 1 to 524288, 2097152 in all
- amax_history: float32 [4, 16], replicated, may hold values from 20 to 200
Outputs:
- mean_grad: bfloat16 [16384, 128], P('dp')
- block_amax: bfloat16 [16], replicated
The draws below stay inside these ranges and needn't reach their ends.
Inputs may be any that keep to these rules, and one draw needn't show every extreme that they name: `block_len`: every tensor has at least one entry; the lengths sum to 2097152.
All inputs are finite; a program needn't handle non-finite values.
Results may differ from the reference program's by a relative error of at most 0.018.
Values may be sent and summed in bfloat16 or wider, within the bound.
A program may use at most 64 MiB of HBM per device.

```python
import math
import jax
import jax.numpy as jnp
import numpy as np
from jax import lax

ROWS = 16384
BLOCKS = 16
HIST = 4
N_GRP = 4
N_DP = 8
DEVICES = 32


def block_scale(own_key, dims, cuts, least, largest):
    factor_of = 1.0
    for dim, shards_of in cuts:
        draws = jax.random.uniform(jax.random.fold_in(jax.random.fold_in(own_key, 6), dim), (shards_of,), jnp.float32, least / len(cuts), largest / len(cuts))
        factor_of = factor_of * jnp.repeat(jnp.exp(draws), dims[dim] // shards_of).reshape((-1,) + (1,) * (len(dims) - 1 - dim))
    return factor_of


def split_up(count, total, most, lean):
    weights = [(1 << 20) // math.isqrt(rank ** lean) + 1 for rank in range(2, count + 1)]
    surplus, counts = total - most - (count - 1), [1] * (count - 1)
    while surplus > 0:
        candidates = [i for i in range(count - 1) if counts[i] < most]
        mass, budget = sum([weights[i] for i in candidates]), surplus
        for i in candidates:
            extra = min(most - counts[i], max(1, budget * weights[i] // mass), surplus)
            counts[i] = counts[i] + extra
            surplus = surplus - extra
    return np.array([most] + counts)


def uneven(own_key, amount, total, bound, skew):
    if amount == 2:
        one = jax.random.randint(own_key, (), max(1, total - bound), min(bound, total - 1) + 1)
        return jnp.stack([one, total - one])
    lengths = jnp.asarray(split_up(amount, total, bound, skew), jnp.int32)
    couples = (amount - 1) // 2
    giver, sink = lengths[1:1 + 2 * couples:2], lengths[2:2 + 2 * couples:2]
    slack = jnp.minimum(giver - 1, bound - sink)
    passed = jax.random.randint(jax.random.fold_in(own_key, 1), (couples,), 0, 1 << 20) % (slack + 1)
    lengths = lengths.at[1:1 + 2 * couples:2].set(giver - passed).at[2:2 + 2 * couples:2].set(sink + passed)
    return lengths[jax.random.permutation(jax.random.fold_in(own_key, 2), amount)]


def noise(rng, extent, spread, most, shards=(), held_as=jnp.bfloat16):
    entries = spread * jax.random.normal(rng, extent, jnp.float32)
    if shards:
        entries = entries * block_scale(rng, extent, shards, -0.22, 0.18)
    return jnp.clip(entries, -most, most).astype(held_as)


def setup_inputs(seed: int = 0) -> dict:
    key_list = jax.random.split(jax.random.key(seed), 4)
    return {
        "gradients": noise(key_list[0], (N_GRP, N_DP, ROWS, 128), 8.0, 48.0, ((0, 4), (1, 8))),
        "block_len": uneven(key_list[1], BLOCKS, ROWS * 128, ROWS * 32, 2).astype(jnp.int32),
        "amax_history": jnp.clip(jnp.exp(jax.random.uniform(key_list[2], (HIST, BLOCKS), jnp.float32, math.log(20.0), math.log(200.0))), 20.0, 200.0),
    }


SATURATE = 448.0


def reference(gradients, block_len, amax_history):
    block_ends = jnp.cumsum(block_len).astype(jnp.int32)
    position = (jnp.arange(ROWS, dtype=jnp.int32)[:, None] * 128 + jnp.arange(128, dtype=jnp.int32)[None, :])
    block = jnp.sum((position[:, :, None] >= block_ends[None, None, :]).astype(jnp.int32), axis=-1)
    in_block = block[:, :, None] == jnp.arange(BLOCKS, dtype=jnp.int32)[None, None, :]
    scales = SATURATE / jnp.maximum(jnp.max(amax_history, axis=0), 1.0)
    scale_elem = jnp.sum(jnp.where(in_block, scales[None, None, :], jnp.float32(0.0)), axis=-1)

    def one_group(carry, group_grads):
        accumulated, maxima = carry
        summed = jnp.sum(group_grads.astype(jnp.float32), axis=0)
        local_max = jnp.max(jnp.where(in_block, jnp.abs(summed)[:, :, None], jnp.float32(0.0)), axis=(0, 1))
        quantized = jnp.clip(summed * scale_elem, -SATURATE, SATURATE).astype(jnp.bfloat16)
        return (accumulated + quantized.astype(jnp.float32), jnp.maximum(maxima, local_max)), None

    start = (jnp.zeros((ROWS, 128), jnp.float32), jnp.zeros((BLOCKS,), jnp.float32))
    (accumulated, maxima), unused = lax.scan(one_group, start, gradients)
    mean_grad = (accumulated / scale_elem / DEVICES).astype(jnp.bfloat16)
    return mean_grad, maxima.astype(jnp.bfloat16)
```

```python
import functools

import jax
import jax.numpy as jnp
from jax import lax
from jax.experimental import pallas as pl
from jax.experimental.pallas import tpu as pltpu
from jax.sharding import PartitionSpec as P

SATURATE = 448.0
CHUNKS = 16
CORES = 2
LAG_PAIR = 2
LAG_MEAN = 5
LAG_BACK = 7
MESH = pl.DeviceIdType.MESH


def y_extent(dp):
    y = 1
    while (2 * y) * (2 * y) <= dp:
        y *= 2
    return y


def kernel(
    cfg, len_hbm, hist_hbm, grad, out, amax_out,
    len_ref, hist_ref, own, ring, qown, qsib, pair, xbuf, fin_out, fin_in,
    scale_buf, inv_buf, block_buf, acc, msg, maxima,
    small_sem, own_sem, r_send, r_recv, q_send, q_recv, x_send, x_recv,
    f_send, f_recv, m_send, m_recv,
):
    N, grp, Y, Z, K, lines, piece = cfg
    far = N // 2
    X = grp // CORES
    half = lines // CORES
    blocks = len_ref.shape[0]
    hist = hist_ref.shape[0]
    devices = N * grp
    d = lax.axis_index("dp")
    g = lax.axis_index("grp")
    core = g % CORES
    bf, f32 = jnp.bfloat16, jnp.float32

    snake = Y * (Z - 1)

    def place_of(d):
        z, y = d // Y, d % Y
        up = (z + Z - 1) // Z
        odd = y % 2
        along = (z - 1) * (1 - odd) + (Z - 1 - z) * odd
        return up * (y * (Z - 1) + along) + (1 - up) * (snake + Y - 1 - y)

    def device_at(p):
        p = p % N
        back = p // snake
        y = p // (Z - 1)
        r = p % (Z - 1)
        odd = y % 2
        z = 1 + r * (1 - odd) + (Z - 2 - r) * odd
        return (1 - back) * (z * Y + y) + back * (Y - 1 - (p - snake))

    me = place_of(d)
    ahead = (device_at(me + 1), device_at(me + N - 1))

    def slice_at(way, dist):
        return device_at(me + (dist if way == 0 else N - dist))

    def remote(src, dst, send, recv, target):
        return pltpu.make_async_remote_copy(
            src_ref=src, dst_ref=dst, send_sem=send, recv_sem=recv,
            device_id=target, device_id_type=MESH,
        )

    def own_copy(s):
        return pltpu.make_async_copy(grad.at[s], own.at[s], own_sem.at[s])

    def first_hop(way, dist, k):
        return remote(grad.at[slice_at(way, dist), k], ring.at[way, dist - 1, k],
                      r_send.at[k], r_recv.at[way, dist - 1, k], {"dp": ahead[way]})

    def next_hop(way, dist, k):
        return remote(ring.at[way, dist, k], ring.at[way, dist - 1, k],
                      r_send.at[k], r_recv.at[way, dist - 1, k], {"dp": ahead[way]})

    def await_ring(way, dist, k):
        remote(ring.at[way, dist, k], ring.at[way, dist, k], r_send.at[k],
               r_recv.at[way, dist, k], {"dp": ahead[1 - way]}).wait_recv()

    def relay(way, dist, k):
        await_ring(way, dist, k)
        ring[way, dist, k] = ring[way, dist, k] + own[slice_at(way, dist), k]
        next_hop(way, dist, k).start()

    mine = pl.ds(pl.multiple_of(core * half, half), half)
    theirs = pl.ds(pl.multiple_of((CORES - 1 - core) * half, half), half)
    sibling = {"grp": g + CORES - 1 - 2 * core}

    def q_copy(k):
        return remote(qown.at[k, theirs], qsib.at[k], q_send, q_recv.at[k], sibling)

    def x_peer(j):
        return {"grp": (g + CORES * j) % grp}

    def x_copy(k, j):
        return remote(pair.at[k], xbuf.at[k, j - 1], x_send, x_recv.at[k, j - 1], x_peer(j))

    def f_copy(k):
        return remote(fin_out.at[k], fin_in.at[k], f_send, f_recv.at[k], sibling)

    def device(j):
        flat = (d * grp + g + j) % devices
        return {"dp": flat // grp, "grp": flat % grp}

    def m_copy(j):
        return remote(msg, maxima.at[j - 1], m_send, m_recv, device(j))

    def drain(ref, sem):
        pltpu.make_async_copy(ref, ref, sem).wait()

    def each(lower, upper, action):
        def one(i, carry):
            action(i)
            return carry

        lax.fori_loop(lower, upper, one, 0)

    barrier = pltpu.get_barrier_semaphore()
    near = [{"dp": ahead[0]}, {"dp": ahead[1]}, sibling]
    near += [x_peer(j) for j in range(1, X)]
    for target in near:
        pl.semaphore_signal(barrier, inc=1, device_id=target, device_id_type=MESH)
    len_copy = pltpu.make_async_copy(len_hbm, len_ref, small_sem.at[0])
    hist_copy = pltpu.make_async_copy(hist_hbm, hist_ref, small_sem.at[1])
    len_copy.start()
    hist_copy.start()
    each(0, N, lambda s: own_copy(s).start())
    pl.semaphore_wait(barrier, len(near))

    def start_far(m):
        first_hop(0, far, 2 * m).start()
        first_hop(1, far, 2 * m + 1).start()

    each(0, K // 2, start_far)

    acc[...] = jnp.zeros(acc.shape, f32)
    len_copy.wait()
    hist_copy.wait()
    ends = []
    factors = []
    total = jnp.int32(0)
    for c in range(blocks):
        total = total + len_ref[c]
        ends.append(total)
        top = hist_ref[0, c]
        for h in range(1, hist):
            top = jnp.maximum(top, hist_ref[h, c])
        top = jnp.maximum(jnp.full((8, 128), top, f32), 1.0)
        factors.append((SATURATE / top, top * (1.0 / (SATURATE * devices))))

    each(0, N, lambda s: own_copy(s).wait())

    def second(m):
        if far > 1:
            relay(0, far - 1, 2 * m)
            first_hop(1, far - 1, 2 * m).start()
            first_hop(0, far - 1, 2 * m + 1).start()
            relay(1, far - 1, 2 * m + 1)

    each(0, K // 2, second)

    def prepare(i):
        shape = (piece // 8, 8, 128)
        at = (
            lax.broadcasted_iota(jnp.int32, shape, 0) * 1024
            + lax.broadcasted_iota(jnp.int32, shape, 1) * 128
            + lax.broadcasted_iota(jnp.int32, shape, 2)
        ) + (d * (K * lines) + i * piece) * 128
        block = jnp.zeros(shape, jnp.int32)
        scale = jnp.broadcast_to(factors[0][0][None], shape)
        inv = jnp.broadcast_to(factors[0][1][None], shape)
        for c in range(1, blocks):
            after = at >= ends[c - 1]
            block = jnp.where(after, c, block)
            scale = jnp.where(after, factors[c][0][None], scale)
            inv = jnp.where(after, factors[c][1][None], inv)
        rows = pl.ds(pl.multiple_of(i * piece, piece), piece)
        block_buf[rows] = block.reshape(piece, 128)
        scale_buf[rows] = scale.reshape(piece, 128)
        inv_buf[rows] = inv.reshape(piece, 128)

    each(0, K * lines // piece, prepare)

    def phase(h, carry):
        dist = far - h

        def one(k, carry):
            relay(0, dist, k)
            relay(1, dist, k)
            return carry

        return lax.fori_loop(0, K, one, carry)

    lax.fori_loop(2, far, phase, 0)

    def stage_q(k):
        await_ring(0, 0, k)
        await_ring(1, 0, k)

        def step(i, tops):
            rows = pl.ds(pl.multiple_of(i * piece, piece), piece)
            flat = pl.ds(pl.multiple_of(k * lines + i * piece, piece), piece)
            value = own[d, k, rows].astype(f32)
            value = value + ring[0, 0, k, rows].astype(f32) + ring[1, 0, k, rows].astype(f32)
            quant = jnp.clip(value * scale_buf[flat], -SATURATE, SATURATE)
            qown[k, rows] = quant.astype(bf)
            size = jnp.abs(value).reshape(piece // 8, 8, 128)
            block = block_buf[flat].reshape(piece // 8, 8, 128)
            return tuple(
                jnp.maximum(tops[c], jnp.max(jnp.where(block == c, size, 0.0), axis=0))
                for c in range(blocks)
            )

        tops = lax.fori_loop(0, lines // piece, step, tuple(acc[c] for c in range(blocks)))
        q_copy(k).start()
        for c in range(blocks):
            acc[c] = tops[c]

    def stage_pair(k):
        q_copy(k).wait_recv()
        pair[k] = (qown[k, mine].astype(f32) + qsib[k].astype(f32)).astype(bf)
        for j in range(1, X):
            x_copy(k, j).start()

    def stage_mean(k):
        value = pair[k].astype(f32)
        for j in range(1, X):
            x_copy(k, j).wait_recv()
            value = value + xbuf[k, j - 1].astype(f32)
        rows = pl.ds(pl.multiple_of(k * lines + core * half, half), half)
        mean = (value * inv_buf[rows]).astype(bf)
        out[k, mine] = mean
        fin_out[k] = mean
        f_copy(k).start()

    def stage_back(k):
        f_copy(k).wait_recv()
        out[k, theirs] = fin_in[k]

    def stage_max():
        top = jnp.max(acc[...], axis=1)
        top = jnp.max(top, axis=1, keepdims=True)
        lane = lax.broadcasted_iota(jnp.int32, (blocks, 128), 1)
        row = lax.broadcasted_iota(jnp.int32, (blocks, 128), 0)
        msg[...] = jnp.max(jnp.where(lane == row, top, 0.0), axis=0, keepdims=True)
        each(1, devices, lambda j: m_copy(j).start())

    def tick(t, carry):
        @pl.when(t < K)
        def _():
            stage_q(t)

        @pl.when(t == K - 1)
        def _():
            stage_max()

        @pl.when((t >= LAG_PAIR) & (t < K + LAG_PAIR))
        def _():
            stage_pair(t - LAG_PAIR)

        @pl.when((t >= LAG_MEAN) & (t < K + LAG_MEAN))
        def _():
            stage_mean(t - LAG_MEAN)

        @pl.when(t >= LAG_BACK)
        def _():
            k = t - LAG_BACK
            stage_back(k)
            drain(own.at[pl.ds(0, N - 1), k], r_send.at[k])

        return carry

    lax.fori_loop(0, K + LAG_BACK, tick, 0)

    drain(maxima, m_recv)
    top = jnp.maximum(jnp.max(maxima[...], axis=0), msg[...])
    amax_out[...] = jnp.broadcast_to(top, amax_out.shape).astype(bf)
    drain(maxima, m_send)
    drain(qsib, q_send)
    drain(xbuf, x_send)
    drain(fin_in, f_send)


def body(gradients, block_len, amax_history):
    dp = lax.axis_size("dp")
    grp = lax.axis_size("grp")
    rows, lanes = gradients.shape[2:]
    Y = y_extent(dp)
    Z = dp // Y
    K = min(CHUNKS, rows // dp // 32)
    lines = rows // dp // K
    half = lines // CORES
    piece = min(32, lines)
    far = dp // 2
    X = grp // CORES
    cfg = (dp, grp, Y, Z, K, lines, piece)
    bf, f32 = jnp.bfloat16, jnp.float32
    dma = pltpu.SemaphoreType.DMA
    tile = (lines, lanes)
    part = (half, lanes)
    scratch = [
        pltpu.SMEM(block_len.shape, jnp.int32),
        pltpu.SMEM(amax_history.shape, f32),
        pltpu.VMEM((dp, K) + tile, bf),
        pltpu.VMEM((2, far, K) + tile, bf),
        pltpu.VMEM((K,) + tile, bf),
        pltpu.VMEM((K,) + part, bf),
        pltpu.VMEM((K,) + part, bf),
        pltpu.VMEM((K, X - 1) + part, bf),
        pltpu.VMEM((K,) + part, bf),
        pltpu.VMEM((K,) + part, bf),
        pltpu.VMEM((rows // dp, lanes), f32),
        pltpu.VMEM((rows // dp, lanes), f32),
        pltpu.VMEM((rows // dp, lanes), jnp.int32),
        pltpu.VMEM((block_len.shape[0], 8, lanes), f32),
        pltpu.VMEM((1, lanes), f32),
        pltpu.VMEM((dp * grp - 1, 1, lanes), f32),
        dma((2,)),
        dma((dp,)),
        dma((K,)), dma((2, far, K)),
        dma(()), dma((K,)),
        dma(()), dma((K, X - 1)),
        dma(()), dma((K,)),
        dma(()), dma(()),
    ]
    hbm = pl.BlockSpec(memory_space=pltpu.HBM)
    vmem = pl.BlockSpec(memory_space=pltpu.VMEM)
    pinned = [
        pltpu.with_memory_space_constraint(a, pltpu.HBM)
        for a in (block_len, amax_history, gradients.reshape((dp, K) + tile))
    ]
    mean, top = pl.pallas_call(
        functools.partial(kernel, cfg),
        out_shape=(
            jax.ShapeDtypeStruct((K,) + tile, bf),
            jax.ShapeDtypeStruct((8, lanes), bf),
        ),
        in_specs=[hbm, hbm, hbm],
        out_specs=(vmem, vmem),
        scratch_shapes=scratch,
        compiler_params=pltpu.CompilerParams(
            collective_id=0, has_side_effects=True, vmem_limit_bytes=24 << 20
        ),
    )(*pinned)
    return mean.reshape(rows // dp, lanes), top[0, : block_len.shape[0]]


def solution(mesh):
    placed = (P("grp", "dp", None, None), P(), P())
    return jax.shard_map(
        body, mesh=mesh, in_specs=placed, out_specs=(P("dp", None), P()), check_vma=False
    )
```

```python
import functools

import jax
import jax.numpy as jnp
from jax import lax
from jax.experimental import pallas as pl
from jax.experimental.pallas import tpu as pltpu
from jax.sharding import PartitionSpec as P

SATURATE = 448.0
CHUNKS = 4
SPLIT = 4
DIRECT = 1
CORES = 2
LAG_PAIR = 2
LAG_MEAN = 7
LAG_BACK = 9
MESH = pl.DeviceIdType.MESH


def y_extent(dp):
    y = 1
    while (2 * y) * (2 * y) <= dp:
        y *= 2
    return y


def kernel(
    cfg, len_hbm, hist_hbm, grad, out, amax_out,
    len_ref, hist_ref, own, ring, qown, qsib, pair, qall, fin_out, fin_in,
    scale_buf, inv_buf, block_buf, acc, msg, maxima,
    small_sem, own_sem, r_send, r_recv, e_recv, q_send, q_recv, x_send, x_recv,
    f_send, f_recv, d_send, d_recv, m_send, m_recv,
):
    N, grp, Y, Z, K, S, D, lines, piece = cfg
    far = N // 2
    X = grp // CORES
    sub = lines // S
    T = K * S
    half = sub // CORES
    blocks = len_ref.shape[0]
    hist = hist_ref.shape[0]
    devices = N * grp
    d = lax.axis_index("dp")
    g = lax.axis_index("grp")
    core = g % CORES
    bf, f32 = jnp.bfloat16, jnp.float32

    snake = Y * (Z - 1)

    def place_of(d):
        z, y = d // Y, d % Y
        up = (z + Z - 1) // Z
        odd = y % 2
        along = (z - 1) * (1 - odd) + (Z - 1 - z) * odd
        return up * (y * (Z - 1) + along) + (1 - up) * (snake + Y - 1 - y)

    def device_at(p):
        p = p % N
        back = p // snake
        y = p // (Z - 1)
        r = p % (Z - 1)
        odd = y % 2
        z = 1 + r * (1 - odd) + (Z - 2 - r) * odd
        return (1 - back) * (z * Y + y) + back * (Y - 1 - (p - snake))

    me = place_of(d)
    ahead = (device_at(me + 1), device_at(me + N - 1))
    sibling = {"grp": g + CORES - 1 - 2 * core}

    def peer(j):
        return {"grp": (g + j) % grp}

    barrier = pltpu.get_barrier_semaphore()
    near = [{"dp": ahead[0]}, {"dp": ahead[1]}]
    near += [peer(j) for j in range(1, grp)]
    for target in near:
        pl.semaphore_signal(barrier, inc=1, device_id=target, device_id_type=MESH)

    def slice_at(way, dist):
        return device_at(me + (dist if way == 0 else N - dist))

    def span(i, size):
        return pl.ds(pl.multiple_of(i * size, size), size)

    def remote(src, dst, send, recv, target):
        return pltpu.make_async_remote_copy(
            src_ref=src, dst_ref=dst, send_sem=send, recv_sem=recv,
            device_id=target, device_id_type=MESH,
        )

    def own_copy(s):
        return pltpu.make_async_copy(grad.at[s], own.at[s], own_sem.at[s])

    def hop(way, dist, k, src):
        rows = span(k, lines)
        return remote(src.at[rows], ring.at[way, dist - 1, rows], r_send.at[k],
                      r_recv.at[way, dist - 1, k], {"dp": ahead[way]})

    def end_hop(way, t, k, src):
        rows = span(t, sub)
        return remote(src.at[rows], ring.at[way, 0, rows], r_send.at[k],
                      e_recv.at[way, t], {"dp": ahead[way]})

    def await_hop(way, dist, k):
        rows = span(k, lines)
        here = ring.at[way, dist, rows]
        remote(here, here, r_send.at[k], r_recv.at[way, dist, k],
               {"dp": ahead[1 - way]}).wait_recv()

    def await_end(way, t):
        here = ring.at[way, 0, span(t, sub)]
        remote(here, here, r_send.at[t // S], e_recv.at[way, t],
               {"dp": ahead[1 - way]}).wait_recv()

    def first(way, dist, k):
        src = grad.at[slice_at(way, dist)]
        if dist > 1:
            hop(way, dist, k, src).start()
        else:
            for s in range(S):
                end_hop(way, k * S + s, k, src).start()

    def relay(way, dist, k):
        await_hop(way, dist, k)
        rows = span(k, lines)
        ring[way, dist, rows] = ring[way, dist, rows] + own[slice_at(way, dist), rows]
        hop(way, dist, k, ring.at[way, dist]).start()

    def end_relay(way, k):
        await_hop(way, 1, k)
        for s in range(S):
            t = k * S + s
            rows = span(t, sub)
            ring[way, 1, rows] = ring[way, 1, rows] + own[slice_at(way, 1), rows]
            end_hop(way, t, k, ring.at[way, 1]).start()

    def mine(t):
        return pl.ds(pl.multiple_of(t * sub + core * half, half), half)

    def theirs(t):
        return pl.ds(pl.multiple_of(t * sub + (CORES - 1 - core) * half, half), half)

    def q_copy(t):
        return remote(qown.at[theirs(t)], qsib.at[t], q_send, q_recv.at[t], sibling)

    x = g // CORES

    def x_copy(t, j):
        return remote(pair.at[t, x], pair.at[t, x], x_send, x_recv.at[t, j - 1], peer(CORES * j))

    def x_arrival(t, j):
        here = pair.at[t, (x + X - j) % X]
        return remote(here, here, x_send, x_recv.at[t, j - 1], peer(grp - CORES * j))

    def f_copy(t):
        return remote(fin_out.at[t], fin_in.at[t], f_send, f_recv.at[t], sibling)

    def d_copy(t, j):
        i = t - (T - D)
        return remote(qall.at[i, g], qall.at[i, g], d_send, d_recv.at[i, j - 1], peer(j))

    def d_arrival(t, j):
        i = t - (T - D)
        here = qall.at[i, (g + grp - j) % grp]
        return remote(here, here, d_send, d_recv.at[i, j - 1], peer(grp - j))

    def m_copy(j):
        flat = d * grp + g
        to = j + (j - flat + devices) // devices
        slot = flat - (flat - to - 1 + devices) // devices
        return remote(msg, maxima.at[slot], m_send, m_recv,
                      {"dp": to // grp, "grp": to % grp})

    def drain(ref, sem):
        pltpu.make_async_copy(ref, ref, sem).wait()

    def each(lower, upper, action):
        def one(i, carry):
            action(i)
            return carry

        lax.fori_loop(lower, upper, one, 0)

    pl.semaphore_wait(barrier, len(near))

    def start_far(m):
        first(0, far, 2 * m)
        first(1, far, 2 * m + 1)

    each(0, K // 2, start_far)

    len_copy = pltpu.make_async_copy(len_hbm, len_ref, small_sem.at[0])
    hist_copy = pltpu.make_async_copy(hist_hbm, hist_ref, small_sem.at[1])
    len_copy.start()
    hist_copy.start()
    each(0, N, lambda s: own_copy(s).start())
    acc[...] = jnp.zeros(acc.shape, f32)
    len_copy.wait()
    hist_copy.wait()
    ends = []
    factors = []
    total = jnp.int32(0)
    for c in range(blocks):
        total = total + len_ref[c]
        ends.append(total)
        top = hist_ref[0, c]
        for h in range(1, hist):
            top = jnp.maximum(top, hist_ref[h, c])
        top = jnp.maximum(jnp.full((8, 128), top, f32), 1.0)
        factors.append((SATURATE / top, top * (1.0 / (SATURATE * devices))))

    each(0, N, lambda s: own_copy(s).wait())

    def pass_on(way, dist, k):
        if dist == 1:
            end_relay(way, k)
        else:
            relay(way, dist, k)

    def second(m):
        pass_on(0, far - 1, 2 * m)
        first(1, far - 1, 2 * m)
        first(0, far - 1, 2 * m + 1)
        pass_on(1, far - 1, 2 * m + 1)

    each(0, K // 2, second)

    def prepare(i):
        shape = (piece // 8, 8, 128)
        at = (
            lax.broadcasted_iota(jnp.int32, shape, 0) * 1024
            + lax.broadcasted_iota(jnp.int32, shape, 1) * 128
            + lax.broadcasted_iota(jnp.int32, shape, 2)
        ) + (d * (K * lines) + i * piece) * 128
        block = jnp.zeros(shape, jnp.int32)
        scale = jnp.broadcast_to(factors[0][0][None], shape)
        inv = jnp.broadcast_to(factors[0][1][None], shape)
        for c in range(1, blocks):
            after = at >= ends[c - 1]
            block = jnp.where(after, c, block)
            scale = jnp.where(after, factors[c][0][None], scale)
            inv = jnp.where(after, factors[c][1][None], inv)
        rows = span(i, piece)
        block_buf[rows] = block.reshape(piece, 128)
        scale_buf[rows] = scale.reshape(piece, 128)
        inv_buf[rows] = inv.reshape(piece, 128)

    each(0, K * lines // piece, prepare)

    def phase(h, carry):
        dist = far - h

        def one(k, carry):
            relay(0, dist, k)
            relay(1, dist, k)
            return carry

        return lax.fori_loop(0, K, one, carry)

    if far > 2:
        lax.fori_loop(2, far - 1, phase, 0)

        def last_phase(k):
            end_relay(0, k)
            end_relay(1, k)

        each(0, K, last_phase)

    def stage_q(t):
        await_end(0, t)
        await_end(1, t)

        def step(i, tops):
            rows = pl.ds(pl.multiple_of(t * sub + i * piece, piece), piece)
            value = own[d, rows].astype(f32)
            value = value + ring[0, 0, rows].astype(f32) + ring[1, 0, rows].astype(f32)
            quant = jnp.clip(value * scale_buf[rows], -SATURATE, SATURATE)
            qown[rows] = quant.astype(bf)
            size = jnp.abs(value).reshape(piece // 8, 8, 128)
            block = block_buf[rows].reshape(piece // 8, 8, 128)
            return tuple(
                jnp.maximum(tops[c], jnp.max(jnp.where(block == c, size, 0.0), axis=0))
                for c in range(blocks)
            )

        tops = lax.fori_loop(0, sub // piece, step, tuple(acc[c] for c in range(blocks)))

        @pl.when(t < T - D)
        def _():
            q_copy(t).start()

        @pl.when(t >= T - D)
        def _():
            qall[t - (T - D), g] = qown[span(t, sub)]
            for j in range(1, grp):
                d_copy(t, j).start()

        for c in range(blocks):
            acc[c] = tops[c]

    def stage_pair(t):
        q_copy(t).wait_recv()
        pair[t, x] = (qown[mine(t)].astype(f32) + qsib[t].astype(f32)).astype(bf)
        for j in range(1, X):
            x_copy(t, j).start()

    def stage_mean(t):
        for j in range(1, X):
            x_arrival(t, j).wait_recv()
        value = pair[t, 0].astype(f32)
        for j in range(1, X):
            value = value + pair[t, j].astype(f32)
        mean = (value * inv_buf[mine(t)]).astype(bf)
        out[mine(t)] = mean
        fin_out[t] = mean
        f_copy(t).start()

    def stage_back(t):
        f_copy(t).wait_recv()
        out[theirs(t)] = fin_in[t]

    def stage_direct(t):
        for j in range(1, grp):
            d_arrival(t, j).wait_recv()
        i = t - (T - D)
        value = qall[i, 0].astype(f32)
        for j in range(1, grp):
            value = value + qall[i, j].astype(f32)
        rows = span(t, sub)
        out[rows] = (value * inv_buf[rows]).astype(bf)

    def stage_max():
        top = jnp.max(acc[...], axis=1)
        top = jnp.max(top, axis=1, keepdims=True)
        lane = lax.broadcasted_iota(jnp.int32, (blocks, 128), 1)
        row = lax.broadcasted_iota(jnp.int32, (blocks, 128), 0)
        msg[...] = jnp.max(jnp.where(lane == row, top, 0.0), axis=0, keepdims=True)
        each(0, devices - 1, lambda j: m_copy(j).start())

    def tick(t, carry):
        @pl.when(t < T)
        def _():
            stage_q(t)

        @pl.when(t == T - 1)
        def _():
            stage_max()

        @pl.when((t >= LAG_PAIR) & (t < T - D + LAG_PAIR))
        def _():
            stage_pair(t - LAG_PAIR)

        @pl.when((t >= LAG_MEAN) & (t < T - D + LAG_MEAN))
        def _():
            stage_mean(t - LAG_MEAN)

        @pl.when(t >= LAG_BACK)
        def _():
            stage_back(t - LAG_BACK)

        return carry

    lax.fori_loop(0, T - D + LAG_BACK, tick, 0)
    each(0, K, lambda k: drain(own.at[pl.ds(0, N - 1), span(k, lines)], r_send.at[k]))
    for t in range(T - D, T):
        stage_direct(t)

    drain(qsib, q_send)
    drain(fin_in, f_send)
    for j in range(1, X):
        drain(qsib, x_send)
    for j in range(1, grp):
        drain(qall.at[:, 0], d_send)
    drain(maxima, m_recv)
    top = jnp.maximum(jnp.max(maxima[...], axis=0), msg[...])
    amax_out[...] = top[0, :blocks].astype(bf)
    drain(maxima, m_send)


def put_out(mean, top, mean_out, top_out, sem):
    copies = [
        pltpu.make_async_copy(mean, mean_out, sem.at[0]),
        pltpu.make_async_copy(top, top_out, sem.at[1]),
    ]
    for copy in copies:
        copy.start()
    for copy in copies:
        copy.wait()


def body(gradients, block_len, amax_history):
    dp = lax.axis_size("dp")
    grp = lax.axis_size("grp")
    rows, lanes = gradients.shape[2:]
    own_rows = rows // dp
    Y = y_extent(dp)
    Z = dp // Y
    S, D = SPLIT, DIRECT
    K = min(CHUNKS, own_rows // (32 * S))
    T = K * S
    lines = own_rows // K
    sub = lines // S
    half = sub // CORES
    piece = min(32, sub)
    far = dp // 2
    X = grp // CORES
    blocks = block_len.shape[0]
    cfg = (dp, grp, Y, Z, K, S, D, lines, piece)
    bf, f32 = jnp.bfloat16, jnp.float32
    dma = pltpu.SemaphoreType.DMA
    part = (half, lanes)
    scratch = [
        pltpu.SMEM(block_len.shape, jnp.int32),
        pltpu.SMEM(amax_history.shape, f32),
        pltpu.VMEM((dp, own_rows, lanes), bf),
        pltpu.VMEM((2, far, own_rows, lanes), bf),
        pltpu.VMEM((own_rows, lanes), bf),
        pltpu.VMEM((T - D,) + part, bf),
        pltpu.VMEM((T - D, X) + part, bf),
        pltpu.VMEM((D, grp, sub, lanes), bf),
        pltpu.VMEM((T - D,) + part, bf),
        pltpu.VMEM((T - D,) + part, bf),
        pltpu.VMEM((own_rows, lanes), f32),
        pltpu.VMEM((own_rows, lanes), f32),
        pltpu.VMEM((own_rows, lanes), jnp.int32),
        pltpu.VMEM((blocks, 8, lanes), f32),
        pltpu.VMEM((1, lanes), f32),
        pltpu.VMEM((dp * grp - 1, 1, lanes), f32),
        dma((2,)),
        dma((dp,)),
        dma((K,)), dma((2, far, K)), dma((2, T)),
        dma(()), dma((T - D,)),
        dma(()), dma((T - D, X - 1)),
        dma(()), dma((T - D,)),
        dma(()), dma((D, grp - 1)),
        dma(()), dma(()),
    ]
    hbm = pl.BlockSpec(memory_space=pltpu.HBM)
    vmem = pl.BlockSpec(memory_space=pltpu.VMEM)
    anywhere = pl.BlockSpec(memory_space=pl.ANY)
    pinned = [
        pltpu.with_memory_space_constraint(a, pltpu.HBM)
        for a in (block_len, amax_history, gradients.reshape((dp, own_rows, lanes)))
    ]
    shapes = (
        jax.ShapeDtypeStruct((own_rows, lanes), bf),
        jax.ShapeDtypeStruct((blocks,), bf),
    )
    mean, top = pl.pallas_call(
        functools.partial(kernel, cfg),
        out_shape=shapes,
        in_specs=[hbm, hbm, hbm],
        out_specs=(vmem, vmem),
        scratch_shapes=scratch,
        compiler_params=pltpu.CompilerParams(
            collective_id=0, has_side_effects=True, vmem_limit_bytes=24 << 20
        ),
    )(*pinned)
    return pl.pallas_call(
        put_out,
        out_shape=shapes,
        in_specs=[anywhere, anywhere],
        out_specs=(hbm, hbm),
        scratch_shapes=[dma((2,))],
        compiler_params=pltpu.CompilerParams(vmem_limit_bytes=24 << 20),
    )(mean, top)


def solution(mesh):
    placed = (P("grp", "dp", None, None), P(), P())
    return jax.shard_map(
        body, mesh=mesh, in_specs=placed, out_specs=(P("dp", None), P()), check_vma=False
    )
```

```python
import functools

import jax
import jax.numpy as jnp
from jax import lax
from jax.experimental import pallas as pl
from jax.experimental.pallas import tpu as pltpu
from jax.sharding import PartitionSpec as P

SATURATE = 448.0
CHUNKS = 4
SPLIT = 4
DIRECT = 1
SHARED = 2
CORES = 2
LAG_PAIR = 2
LAG_MEAN = 7
LAG_BACK = 9
MESH = pl.DeviceIdType.MESH


def y_extent(dp):
    y = 1
    while (2 * y) * (2 * y) <= dp:
        y *= 2
    return y


def kernel(
    cfg, len_hbm, hist_hbm, grad, out, amax_out,
    len_ref, hist_ref, own, ring, qown, qsib, pair, qall, pall, fin_out, fin_in,
    scale_buf, inv_buf, block_buf, acc, msg, maxima,
    small_sem, own_sem, r_send, r_recv, e_recv, q_send, q_recv, x_send, x_recv,
    f_send, f_recv, d_send, d_recv, p_send, p_recv, m_send, m_recv,
):
    N, grp, Y, Z, K, S, D, E, lines, piece = cfg
    far = N // 2
    X = grp // CORES
    sub = lines // S
    T = K * S
    Q = T - D - E
    half = sub // CORES
    blocks = len_ref.shape[0]
    hist = hist_ref.shape[0]
    devices = N * grp
    d = lax.axis_index("dp")
    g = lax.axis_index("grp")
    core = g % CORES
    bf, f32 = jnp.bfloat16, jnp.float32

    snake = Y * (Z - 1)

    def place_of(d):
        z, y = d // Y, d % Y
        up = (z + Z - 1) // Z
        odd = y % 2
        along = (z - 1) * (1 - odd) + (Z - 1 - z) * odd
        return up * (y * (Z - 1) + along) + (1 - up) * (snake + Y - 1 - y)

    def device_at(p):
        p = p % N
        back = p // snake
        y = p // (Z - 1)
        r = p % (Z - 1)
        odd = y % 2
        z = 1 + r * (1 - odd) + (Z - 2 - r) * odd
        return (1 - back) * (z * Y + y) + back * (Y - 1 - (p - snake))

    me = place_of(d)
    ahead = (device_at(me + 1), device_at(me + N - 1))
    sibling = {"grp": g + CORES - 1 - 2 * core}

    def peer(j):
        return {"grp": (g + j) % grp}

    barrier = pltpu.get_barrier_semaphore()
    near = [{"dp": ahead[0]}, {"dp": ahead[1]}]
    near += [peer(j) for j in range(1, grp)]
    for target in near:
        pl.semaphore_signal(barrier, inc=1, device_id=target, device_id_type=MESH)

    def slice_at(way, dist):
        return device_at(me + (dist if way == 0 else N - dist))

    def span(i, size):
        return pl.ds(pl.multiple_of(i * size, size), size)

    def remote(src, dst, send, recv, target):
        return pltpu.make_async_remote_copy(
            src_ref=src, dst_ref=dst, send_sem=send, recv_sem=recv,
            device_id=target, device_id_type=MESH,
        )

    def own_copy(s):
        return pltpu.make_async_copy(grad.at[s], own.at[s], own_sem.at[s])

    def hop(way, dist, k, src):
        rows = span(k, lines)
        return remote(src.at[rows], ring.at[way, dist - 1, rows], r_send.at[k],
                      r_recv.at[way, dist - 1, k], {"dp": ahead[way]})

    def end_hop(way, t, k, src):
        rows = span(t, sub)
        return remote(src.at[rows], ring.at[way, 0, rows], r_send.at[k],
                      e_recv.at[way, t], {"dp": ahead[way]})

    def await_hop(way, dist, k):
        rows = span(k, lines)
        here = ring.at[way, dist, rows]
        remote(here, here, r_send.at[k], r_recv.at[way, dist, k],
               {"dp": ahead[1 - way]}).wait_recv()

    def await_end(way, t):
        here = ring.at[way, 0, span(t, sub)]
        remote(here, here, r_send.at[t // S], e_recv.at[way, t],
               {"dp": ahead[1 - way]}).wait_recv()

    def first(way, dist, k):
        src = grad.at[slice_at(way, dist)]
        if dist > 1:
            hop(way, dist, k, src).start()
        else:
            for s in range(S):
                end_hop(way, k * S + s, k, src).start()

    def relay(way, dist, k):
        await_hop(way, dist, k)
        rows = span(k, lines)
        ring[way, dist, rows] = ring[way, dist, rows] + own[slice_at(way, dist), rows]
        hop(way, dist, k, ring.at[way, dist]).start()

    def end_relay(way, k):
        await_hop(way, 1, k)
        for s in range(S):
            t = k * S + s
            rows = span(t, sub)
            ring[way, 1, rows] = ring[way, 1, rows] + own[slice_at(way, 1), rows]
            end_hop(way, t, k, ring.at[way, 1]).start()

    def mine(t):
        return pl.ds(pl.multiple_of(t * sub + core * half, half), half)

    def theirs(t):
        return pl.ds(pl.multiple_of(t * sub + (CORES - 1 - core) * half, half), half)

    def q_copy(t):
        return remote(qown.at[theirs(t)], qsib.at[t], q_send, q_recv.at[t], sibling)

    x = g // CORES

    def x_copy(t, j):
        return remote(pair.at[t, x], pair.at[t, x], x_send, x_recv.at[t, j - 1], peer(CORES * j))

    def x_arrival(t, j):
        here = pair.at[t, (x + X - j) % X]
        return remote(here, here, x_send, x_recv.at[t, j - 1], peer(grp - CORES * j))

    def f_copy(t):
        return remote(fin_out.at[t], fin_in.at[t], f_send, f_recv.at[t], sibling)

    def d_copy(t, j):
        i = t - (T - D)
        return remote(qall.at[i, g], qall.at[i, g], d_send, d_recv.at[i, j - 1], peer(j))

    def d_arrival(t, j):
        i = t - (T - D)
        here = qall.at[i, (g + grp - j) % grp]
        return remote(here, here, d_send, d_recv.at[i, j - 1], peer(grp - j))

    def p_copy(t, j):
        here = pall.at[t - Q, core, x]
        return remote(here, here, p_send, p_recv.at[t - Q, j - 1], peer(j))

    def p_arrival(t, j):
        other = (g + grp - j) % grp
        here = pall.at[t - Q, other % CORES, other // CORES]
        return remote(here, here, p_send, p_recv.at[t - Q, j - 1], peer(grp - j))

    def m_copy(i, j):
        return remote(msg, maxima.at[i * grp + j - 1], m_send, m_recv,
                      {"dp": (d + i) % N, "grp": (g + j) % grp})

    def send_max():
        for j in range(1, grp):
            m_copy(0, j).start()

        def one(i):
            for j in range(grp):
                m_copy(i, j).start()

        each(1, N, one)

    def drain(ref, sem):
        pltpu.make_async_copy(ref, ref, sem).wait()

    def each(lower, upper, action):
        def one(i, carry):
            action(i)
            return carry

        lax.fori_loop(lower, upper, one, 0)

    pl.semaphore_wait(barrier, len(near))

    def start_far(m):
        first(0, far, 2 * m)
        first(1, far, 2 * m + 1)

    each(0, K // 2, start_far)

    len_copy = pltpu.make_async_copy(len_hbm, len_ref, small_sem.at[0])
    hist_copy = pltpu.make_async_copy(hist_hbm, hist_ref, small_sem.at[1])
    len_copy.start()
    hist_copy.start()
    each(0, N, lambda s: own_copy(s).start())
    acc[...] = jnp.zeros(acc.shape, f32)
    len_copy.wait()
    hist_copy.wait()
    ends = []
    factors = []
    total = jnp.int32(0)
    for c in range(blocks):
        total = total + len_ref[c]
        ends.append(total)
        top = hist_ref[0, c]
        for h in range(1, hist):
            top = jnp.maximum(top, hist_ref[h, c])
        top = jnp.maximum(jnp.full((8, 128), top, f32), 1.0)
        factors.append((SATURATE / top, top * (1.0 / (SATURATE * devices))))

    each(0, N, lambda s: own_copy(s).wait())

    def pass_on(way, dist, k):
        if dist == 1:
            end_relay(way, k)
        else:
            relay(way, dist, k)

    def second(m):
        pass_on(0, far - 1, 2 * m)
        first(1, far - 1, 2 * m)
        first(0, far - 1, 2 * m + 1)
        pass_on(1, far - 1, 2 * m + 1)

    each(0, K // 2, second)

    def prepare(i):
        shape = (piece // 8, 8, 128)
        at = (
            lax.broadcasted_iota(jnp.int32, shape, 0) * 1024
            + lax.broadcasted_iota(jnp.int32, shape, 1) * 128
            + lax.broadcasted_iota(jnp.int32, shape, 2)
        ) + (d * (K * lines) + i * piece) * 128
        block = jnp.zeros(shape, jnp.int32)
        scale = jnp.broadcast_to(factors[0][0][None], shape)
        inv = jnp.broadcast_to(factors[0][1][None], shape)
        for c in range(1, blocks):
            after = at >= ends[c - 1]
            block = jnp.where(after, c, block)
            scale = jnp.where(after, factors[c][0][None], scale)
            inv = jnp.where(after, factors[c][1][None], inv)
        rows = span(i, piece)
        block_buf[rows] = block.reshape(piece, 128)
        scale_buf[rows] = scale.reshape(piece, 128)
        inv_buf[rows] = inv.reshape(piece, 128)

    each(0, K * lines // piece, prepare)

    def phase(h, carry):
        dist = far - h

        def one(k, carry):
            relay(0, dist, k)
            relay(1, dist, k)
            return carry

        return lax.fori_loop(0, K, one, carry)

    if far > 2:
        lax.fori_loop(2, far - 1, phase, 0)

        def last_phase(k):
            end_relay(0, k)
            end_relay(1, k)

        each(0, K, last_phase)

    def stage_q(t):
        await_end(0, t)
        await_end(1, t)

        def step(i, tops):
            rows = pl.ds(pl.multiple_of(t * sub + i * piece, piece), piece)
            value = own[d, rows].astype(f32)
            value = value + ring[0, 0, rows].astype(f32) + ring[1, 0, rows].astype(f32)
            quant = jnp.clip(value * scale_buf[rows], -SATURATE, SATURATE)
            qown[rows] = quant.astype(bf)
            size = jnp.abs(value).reshape(piece // 8, 8, 128)
            block = block_buf[rows].reshape(piece // 8, 8, 128)
            return tuple(
                jnp.maximum(tops[c], jnp.max(jnp.where(block == c, size, 0.0), axis=0))
                for c in range(blocks)
            )

        tops = lax.fori_loop(0, sub // piece, step, tuple(acc[c] for c in range(blocks)))

        @pl.when(t < T - D)
        def _():
            q_copy(t).start()

        @pl.when(t >= T - D)
        def _():
            qall[t - (T - D), g] = qown[span(t, sub)]
            for j in range(1, grp):
                d_copy(t, j).start()

        for c in range(blocks):
            acc[c] = tops[c]

    def stage_pair(t):
        q_copy(t).wait_recv()
        both = (qown[mine(t)].astype(f32) + qsib[t].astype(f32)).astype(bf)

        @pl.when(t < Q)
        def _():
            pair[t, x] = both
            for j in range(1, X):
                x_copy(t, j).start()

        @pl.when(t >= Q)
        def _():
            pall[t - Q, core, x] = both
            for j in range(1, grp):
                p_copy(t, j).start()

    def stage_mean(t):
        for j in range(1, X):
            x_arrival(t, j).wait_recv()
        value = pair[t, 0].astype(f32)
        for j in range(1, X):
            value = value + pair[t, j].astype(f32)
        mean = (value * inv_buf[mine(t)]).astype(bf)
        out[mine(t)] = mean
        fin_out[t] = mean
        f_copy(t).start()

    def stage_back(t):
        f_copy(t).wait_recv()
        out[theirs(t)] = fin_in[t]

    def stage_shared(t):
        for j in range(1, grp):
            p_arrival(t, j).wait_recv()
        for c in range(CORES):
            value = pall[t - Q, c, 0].astype(f32)
            for j in range(1, X):
                value = value + pall[t - Q, c, j].astype(f32)
            rows = pl.ds(pl.multiple_of(t * sub + c * half, half), half)
            out[rows] = (value * inv_buf[rows]).astype(bf)

    def stage_direct(t):
        for j in range(1, grp):
            d_arrival(t, j).wait_recv()
        i = t - (T - D)
        value = qall[i, 0].astype(f32)
        for j in range(1, grp):
            value = value + qall[i, j].astype(f32)
        rows = span(t, sub)
        out[rows] = (value * inv_buf[rows]).astype(bf)

    def stage_max():
        top = jnp.max(acc[...], axis=1)
        top = jnp.max(top, axis=1, keepdims=True)
        lane = lax.broadcasted_iota(jnp.int32, (blocks, 128), 1)
        row = lax.broadcasted_iota(jnp.int32, (blocks, 128), 0)
        msg[...] = jnp.max(jnp.where(lane == row, top, 0.0), axis=0, keepdims=True)
        send_max()

    def tick(t, carry):
        @pl.when(t < T)
        def _():
            stage_q(t)

        @pl.when(t == T - 1)
        def _():
            stage_max()

        @pl.when((t >= LAG_PAIR) & (t < T - D + LAG_PAIR))
        def _():
            stage_pair(t - LAG_PAIR)

        @pl.when((t >= LAG_MEAN) & (t < Q + LAG_MEAN))
        def _():
            stage_mean(t - LAG_MEAN)

        @pl.when((t >= LAG_BACK) & (t < Q + LAG_BACK))
        def _():
            stage_back(t - LAG_BACK)

        return carry

    lax.fori_loop(0, max(Q + LAG_BACK, T - D + LAG_PAIR), tick, 0)
    each(0, K, lambda k: drain(own.at[pl.ds(0, N - 1), span(k, lines)], r_send.at[k]))
    for t in range(Q, T - D):
        stage_shared(t)
    for t in range(T - D, T):
        stage_direct(t)

    drain(qsib, q_send)
    drain(fin_in, f_send)
    for j in range(1, X):
        drain(fin_in, x_send)
    for j in range(1, grp):
        drain(qall.at[:, 0], d_send)
        drain(pall.at[:, 0, 0], p_send)
    drain(maxima, m_recv)
    top = jnp.maximum(jnp.max(maxima[...], axis=0), msg[...])
    amax_out[...] = top[0, :blocks].astype(bf)
    drain(maxima, m_send)


def put_out(mean, top, mean_out, top_out, sem):
    copies = [
        pltpu.make_async_copy(mean, mean_out, sem.at[0]),
        pltpu.make_async_copy(top, top_out, sem.at[1]),
    ]
    for copy in copies:
        copy.start()
    for copy in copies:
        copy.wait()


def body(gradients, block_len, amax_history):
    dp = lax.axis_size("dp")
    grp = lax.axis_size("grp")
    rows, lanes = gradients.shape[2:]
    own_rows = rows // dp
    Y = y_extent(dp)
    Z = dp // Y
    S, D, E = SPLIT, DIRECT, SHARED
    K = min(CHUNKS, own_rows // (32 * S))
    T = K * S
    lines = own_rows // K
    sub = lines // S
    half = sub // CORES
    piece = min(64, sub)
    far = dp // 2
    X = grp // CORES
    blocks = block_len.shape[0]
    Q = T - D - E
    cfg = (dp, grp, Y, Z, K, S, D, E, lines, piece)
    bf, f32 = jnp.bfloat16, jnp.float32
    dma = pltpu.SemaphoreType.DMA
    part = (half, lanes)
    scratch = [
        pltpu.SMEM(block_len.shape, jnp.int32),
        pltpu.SMEM(amax_history.shape, f32),
        pltpu.VMEM((dp, own_rows, lanes), bf),
        pltpu.VMEM((2, far, own_rows, lanes), bf),
        pltpu.VMEM((own_rows, lanes), bf),
        pltpu.VMEM((T - D,) + part, bf),
        pltpu.VMEM((Q, X) + part, bf),
        pltpu.VMEM((D, grp, sub, lanes), bf),
        pltpu.VMEM((E, CORES, X) + part, bf),
        pltpu.VMEM((Q,) + part, bf),
        pltpu.VMEM((Q,) + part, bf),
        pltpu.VMEM((own_rows, lanes), f32),
        pltpu.VMEM((own_rows, lanes), f32),
        pltpu.VMEM((own_rows, lanes), jnp.int32),
        pltpu.VMEM((blocks, 8, lanes), f32),
        pltpu.VMEM((1, lanes), f32),
        pltpu.VMEM((dp * grp - 1, 1, lanes), f32),
        dma((2,)),
        dma((dp,)),
        dma((K,)), dma((2, far, K)), dma((2, T)),
        dma(()), dma((T - D,)),
        dma(()), dma((Q, X - 1)),
        dma(()), dma((Q,)),
        dma(()), dma((D, grp - 1)),
        dma(()), dma((E, grp - 1)),
        dma(()), dma(()),
    ]
    hbm = pl.BlockSpec(memory_space=pltpu.HBM)
    vmem = pl.BlockSpec(memory_space=pltpu.VMEM)
    anywhere = pl.BlockSpec(memory_space=pl.ANY)
    pinned = [
        pltpu.with_memory_space_constraint(a, pltpu.HBM)
        for a in (block_len, amax_history, gradients.reshape((dp, own_rows, lanes)))
    ]
    shapes = (
        jax.ShapeDtypeStruct((own_rows, lanes), bf),
        jax.ShapeDtypeStruct((blocks,), bf),
    )
    mean, top = pl.pallas_call(
        functools.partial(kernel, cfg),
        out_shape=shapes,
        in_specs=[hbm, hbm, hbm],
        out_specs=(vmem, vmem),
        scratch_shapes=scratch,
        compiler_params=pltpu.CompilerParams(
            collective_id=0, has_side_effects=True, vmem_limit_bytes=24 << 20
        ),
    )(*pinned)
    return pl.pallas_call(
        put_out,
        out_shape=shapes,
        in_specs=[anywhere, anywhere],
        out_specs=(hbm, hbm),
        scratch_shapes=[dma((2,))],
        compiler_params=pltpu.CompilerParams(vmem_limit_bytes=24 << 20),
    )(mean, top)


def solution(mesh):
    placed = (P("grp", "dp", None, None), P(), P())
    return jax.shard_map(
        body, mesh=mesh, in_specs=placed, out_specs=(P("dp", None), P()), check_vma=False
    )
```

```python
import functools

import jax
import jax.numpy as jnp
from jax import lax
from jax.experimental import pallas as pl
from jax.experimental.pallas import tpu as pltpu
from jax.sharding import PartitionSpec as P

SATURATE = 448.0
CHUNKS = 4
SPLIT = 4
DIRECT = 1
SHARED = 2
CORES = 2
LAG_PAIR = 2
LAG_MEAN = 7
LAG_BACK = 9
HELD = 4
MESH = pl.DeviceIdType.MESH


def y_extent(dp):
    y = 1
    while (2 * y) * (2 * y) <= dp:
        y *= 2
    return y


def kernel(
    cfg, len_hbm, hist_hbm, grad, out, amax_out,
    len_ref, hist_ref, own, ring, qown, qsib, pair, qall, pall, fin_out, fin_in,
    scale_buf, inv_buf, block_buf, acc, msg, maxima,
    small_sem, own_sem, r_send, r_recv, e_recv, q_send, q_recv, x_send, x_recv,
    f_send, f_recv, d_send, d_recv, p_send, p_recv, m_send, m_recv,
):
    N, grp, Y, Z, K, S, D, E, lines, piece = cfg
    far = N // 2
    X = grp // CORES
    sub = lines // S
    T = K * S
    Q = T - D - E
    half = sub // CORES
    blocks = len_ref.shape[0]
    hist = hist_ref.shape[0]
    devices = N * grp
    d = lax.axis_index("dp")
    g = lax.axis_index("grp")
    core = g % CORES
    bf, f32 = jnp.bfloat16, jnp.float32

    snake = Y * (Z - 1)

    def place_of(d):
        z, y = d // Y, d % Y
        up = (z + Z - 1) // Z
        odd = y % 2
        along = (z - 1) * (1 - odd) + (Z - 1 - z) * odd
        return up * (y * (Z - 1) + along) + (1 - up) * (snake + Y - 1 - y)

    def device_at(p):
        p = p % N
        back = p // snake
        y = p // (Z - 1)
        r = p % (Z - 1)
        odd = y % 2
        z = 1 + r * (1 - odd) + (Z - 2 - r) * odd
        return (1 - back) * (z * Y + y) + back * (Y - 1 - (p - snake))

    me = place_of(d)
    ahead = (device_at(me + 1), device_at(me + N - 1))
    sibling = {"grp": g + CORES - 1 - 2 * core}

    def peer(j):
        return {"grp": (g + j) % grp}

    barrier = pltpu.get_barrier_semaphore()
    near = [{"dp": ahead[0]}, {"dp": ahead[1]}]
    near += [peer(j) for j in range(1, grp)]
    for target in near:
        pl.semaphore_signal(barrier, inc=1, device_id=target, device_id_type=MESH)

    def slice_at(way, dist):
        return device_at(me + (dist if way == 0 else N - dist))

    def span(i, size):
        return pl.ds(pl.multiple_of(i * size, size), size)

    def remote(src, dst, send, recv, target):
        return pltpu.make_async_remote_copy(
            src_ref=src, dst_ref=dst, send_sem=send, recv_sem=recv,
            device_id=target, device_id_type=MESH,
        )

    def own_copy(s):
        return pltpu.make_async_copy(grad.at[s], own.at[s], own_sem.at[s])

    def hop(way, dist, k, src):
        rows = span(k, lines)
        return remote(src.at[rows], ring.at[way, dist - 1, rows], r_send.at[k],
                      r_recv.at[way, dist - 1, k], {"dp": ahead[way]})

    def end_hop(way, t, k, src):
        rows = span(t, sub)
        return remote(src.at[rows], ring.at[way, 0, rows], r_send.at[k],
                      e_recv.at[way, t], {"dp": ahead[way]})

    def await_hop(way, dist, k):
        rows = span(k, lines)
        here = ring.at[way, dist, rows]
        remote(here, here, r_send.at[k], r_recv.at[way, dist, k],
               {"dp": ahead[1 - way]}).wait_recv()

    def await_end(way, t):
        here = ring.at[way, 0, span(t, sub)]
        remote(here, here, r_send.at[t // S], e_recv.at[way, t],
               {"dp": ahead[1 - way]}).wait_recv()

    def first(way, dist, k):
        src = grad.at[slice_at(way, dist)]
        if dist > 1:
            hop(way, dist, k, src).start()
        else:
            for s in range(S):
                end_hop(way, k * S + s, k, src).start()

    def relay(way, dist, k):
        await_hop(way, dist, k)
        rows = span(k, lines)
        ring[way, dist, rows] = ring[way, dist, rows] + own[slice_at(way, dist), rows]
        hop(way, dist, k, ring.at[way, dist]).start()

    def end_relay(way, k):
        await_hop(way, 1, k)
        for s in range(S):
            t = k * S + s
            rows = span(t, sub)
            ring[way, 1, rows] = ring[way, 1, rows] + own[slice_at(way, 1), rows]
            end_hop(way, t, k, ring.at[way, 1]).start()

    def mine(t):
        return pl.ds(pl.multiple_of(t * sub + core * half, half), half)

    def theirs(t):
        return pl.ds(pl.multiple_of(t * sub + (CORES - 1 - core) * half, half), half)

    def q_copy(t):
        return remote(qown.at[theirs(t)], qsib.at[t], q_send, q_recv.at[t], sibling)

    x = g // CORES

    def x_copy(t, j):
        return remote(pair.at[t, x], pair.at[t, x], x_send, x_recv.at[t, j - 1], peer(CORES * j))

    def x_arrival(t, j):
        here = pair.at[t, (x + X - j) % X]
        return remote(here, here, x_send, x_recv.at[t, j - 1], peer(grp - CORES * j))

    def f_copy(t):
        return remote(fin_out.at[t], fin_in.at[t], f_send, f_recv.at[t], sibling)

    def d_copy(t, j):
        i = t - (T - D)
        return remote(qall.at[i, g], qall.at[i, g], d_send, d_recv.at[i, j - 1], peer(j))

    def d_arrival(t, j):
        i = t - (T - D)
        here = qall.at[i, (g + grp - j) % grp]
        return remote(here, here, d_send, d_recv.at[i, j - 1], peer(grp - j))

    def p_copy(t, j):
        here = pall.at[t - Q, core, x]
        return remote(here, here, p_send, p_recv.at[t - Q, j - 1], peer(j))

    def p_arrival(t, j):
        other = (g + grp - j) % grp
        here = pall.at[t - Q, other % CORES, other // CORES]
        return remote(here, here, p_send, p_recv.at[t - Q, j - 1], peer(grp - j))

    def send_max():
        flat = d * grp + g
        maxima[flat] = msg[...]

        def one(i):
            for j in range(grp):
                @pl.when((i != d) | (j != g))
                def _(j=j):
                    remote(msg, maxima.at[flat], m_send, m_recv, {"dp": i, "grp": j}).start()

        each(0, N, one)

    def drain(ref, sem):
        pltpu.make_async_copy(ref, ref, sem).wait()

    def each(lower, upper, action):
        def one(i, carry):
            action(i)
            return carry

        lax.fori_loop(lower, upper, one, 0)

    pl.semaphore_wait(barrier, len(near))

    def start_far(m):
        first(0, far, 2 * m)
        first(1, far, 2 * m + 1)

    each(0, K // 2, start_far)

    len_copy = pltpu.make_async_copy(len_hbm, len_ref, small_sem.at[0])
    hist_copy = pltpu.make_async_copy(hist_hbm, hist_ref, small_sem.at[1])
    len_copy.start()
    hist_copy.start()
    each(0, N, lambda s: own_copy(s).start())
    acc[...] = jnp.zeros(acc.shape, f32)
    len_copy.wait()
    hist_copy.wait()
    ends = []
    factors = []
    total = jnp.int32(0)
    for c in range(blocks):
        total = total + len_ref[c]
        ends.append(total)
        top = hist_ref[0, c]
        for h in range(1, hist):
            top = jnp.maximum(top, hist_ref[h, c])
        top = jnp.maximum(jnp.full((8, 128), top, f32), 1.0)
        factors.append((SATURATE / top, top * (1.0 / (SATURATE * devices))))

    each(0, N, lambda s: own_copy(s).wait())

    def pass_on(way, dist, k):
        if dist == 1:
            end_relay(way, k)
        else:
            relay(way, dist, k)

    def second(m):
        pass_on(0, far - 1, 2 * m)
        first(1, far - 1, 2 * m)
        first(0, far - 1, 2 * m + 1)
        pass_on(1, far - 1, 2 * m + 1)

    each(0, K // 2, second)

    def prepare(i):
        shape = (piece // 8, 8, 128)
        at = (
            lax.broadcasted_iota(jnp.int32, shape, 0) * 1024
            + lax.broadcasted_iota(jnp.int32, shape, 1) * 128
            + lax.broadcasted_iota(jnp.int32, shape, 2)
        ) + (d * (K * lines) + i * piece) * 128
        block = jnp.zeros(shape, jnp.int32)
        scale = jnp.broadcast_to(factors[0][0][None], shape)
        inv = jnp.broadcast_to(factors[0][1][None], shape)
        for c in range(1, blocks):
            after = at >= ends[c - 1]
            block = jnp.where(after, c, block)
            scale = jnp.where(after, factors[c][0][None], scale)
            inv = jnp.where(after, factors[c][1][None], inv)
        rows = span(i, piece)
        block_buf[rows] = block.reshape(piece, 128)
        scale_buf[rows] = scale.reshape(piece, 128)
        inv_buf[rows] = inv.reshape(piece, 128)

    each(0, K * lines // piece, prepare)

    def phase(h, carry):
        dist = far - h

        def one(k, carry):
            relay(0, dist, k)
            relay(1, dist, k)
            return carry

        return lax.fori_loop(0, K, one, carry)

    if far > 2:
        lax.fori_loop(2, far - 1, phase, 0)

        def last_phase(k):
            end_relay(0, k)
            end_relay(1, k)

        each(0, K - 1, last_phase)

        @pl.when(core == 0)
        def _():
            last_phase(K - 1)

    def stage_q(t):
        await_end(0, t)
        await_end(1, t)

        def step(i, tops):
            rows = pl.ds(pl.multiple_of(t * sub + i * piece, piece), piece)
            value = own[d, rows].astype(f32)
            value = value + ring[0, 0, rows].astype(f32) + ring[1, 0, rows].astype(f32)
            quant = jnp.clip(value * scale_buf[rows], -SATURATE, SATURATE)
            qown[rows] = quant.astype(bf)
            size = jnp.abs(value).reshape(piece // 8, 8, 128)
            block = block_buf[rows].reshape(piece // 8, 8, 128)
            return tuple(
                jnp.maximum(tops[c], jnp.max(jnp.where(block == c, size, 0.0), axis=0))
                for c in range(blocks)
            )

        tops = lax.fori_loop(0, sub // piece, step, tuple(acc[c] for c in range(blocks)))

        @pl.when(t < T - D)
        def _():
            q_copy(t).start()

        @pl.when(t >= T - D)
        def _():
            qall[t - (T - D), g] = qown[span(t, sub)]
            for j in range(1, grp):
                d_copy(t, j).start()

        for c in range(blocks):
            acc[c] = tops[c]

    def stage_pair(t):
        q_copy(t).wait_recv()
        both = (qown[mine(t)].astype(f32) + qsib[t].astype(f32)).astype(bf)

        @pl.when(t < Q)
        def _():
            pair[t, x] = both
            for j in range(1, X):
                x_copy(t, j).start()

        @pl.when(t >= Q)
        def _():
            pall[t - Q, core, x] = both
            for j in range(1, grp):
                p_copy(t, j).start()

    def stage_mean(t):
        for j in range(1, X):
            x_arrival(t, j).wait_recv()
        value = pair[t, 0].astype(f32)
        for j in range(1, X):
            value = value + pair[t, j].astype(f32)
        mean = (value * inv_buf[mine(t)]).astype(bf)
        out[mine(t)] = mean
        fin_out[t] = mean
        f_copy(t).start()

    def stage_back(t):
        f_copy(t).wait_recv()
        out[theirs(t)] = fin_in[t]

    def stage_shared(t):
        for j in range(1, grp):
            p_arrival(t, j).wait_recv()
        for c in range(CORES):
            value = pall[t - Q, c, 0].astype(f32)
            for j in range(1, X):
                value = value + pall[t - Q, c, j].astype(f32)
            rows = pl.ds(pl.multiple_of(t * sub + c * half, half), half)
            out[rows] = (value * inv_buf[rows]).astype(bf)

    def stage_direct(t):
        for j in range(1, grp):
            d_arrival(t, j).wait_recv()
        i = t - (T - D)
        value = qall[i, 0].astype(f32)
        for j in range(1, grp):
            value = value + qall[i, j].astype(f32)
        rows = span(t, sub)
        out[rows] = (value * inv_buf[rows]).astype(bf)

    def stage_max():
        top = jnp.max(acc[...], axis=1)
        top = jnp.max(top, axis=1, keepdims=True)
        lane = lax.broadcasted_iota(jnp.int32, (blocks, 128), 1)
        row = lax.broadcasted_iota(jnp.int32, (blocks, 128), 0)
        msg[...] = jnp.max(jnp.where(lane == row, top, 0.0), axis=0, keepdims=True)
        send_max()

    def tick(t, carry):
        if far > 2:
            @pl.when((t == max((K - 1) * S - HELD, 0)) & (core > 0))
            def _():
                end_relay(0, K - 1)
                end_relay(1, K - 1)

        @pl.when(t < T)
        def _():
            stage_q(t)

        @pl.when(t == T - 1)
        def _():
            stage_max()

        @pl.when((t >= LAG_PAIR) & (t < T - D + LAG_PAIR))
        def _():
            stage_pair(t - LAG_PAIR)

        @pl.when((t >= LAG_MEAN) & (t < Q + LAG_MEAN))
        def _():
            stage_mean(t - LAG_MEAN)

        @pl.when((t >= LAG_BACK) & (t < Q + LAG_BACK))
        def _():
            stage_back(t - LAG_BACK)

        return carry

    lax.fori_loop(0, max(Q + LAG_BACK, T - D + LAG_PAIR), tick, 0)
    each(0, K, lambda k: drain(own.at[pl.ds(0, N - 1), span(k, lines)], r_send.at[k]))
    for t in range(Q, T - D):
        stage_shared(t)
    for t in range(T - D, T):
        stage_direct(t)

    drain(qsib, q_send)
    drain(fin_in, f_send)
    for j in range(1, X):
        drain(fin_in, x_send)
    for j in range(1, grp):
        drain(qall.at[:, 0], d_send)
        drain(pall.at[:, 0, 0], p_send)
    drain(maxima.at[pl.ds(0, devices - 1)], m_recv)
    top = jnp.max(maxima[...], axis=0)
    amax_out[...] = top[0, :blocks].astype(bf)
    drain(maxima.at[pl.ds(0, devices - 1)], m_send)


def put_out(mean, top, mean_out, top_out, sem):
    copies = [
        pltpu.make_async_copy(mean, mean_out, sem.at[0]),
        pltpu.make_async_copy(top, top_out, sem.at[1]),
    ]
    for copy in copies:
        copy.start()
    for copy in copies:
        copy.wait()


def body(gradients, block_len, amax_history):
    dp = lax.axis_size("dp")
    grp = lax.axis_size("grp")
    rows, lanes = gradients.shape[2:]
    own_rows = rows // dp
    Y = y_extent(dp)
    Z = dp // Y
    S, D, E = SPLIT, DIRECT, SHARED
    K = min(CHUNKS, own_rows // (32 * S))
    T = K * S
    lines = own_rows // K
    sub = lines // S
    half = sub // CORES
    piece = min(64, sub)
    far = dp // 2
    X = grp // CORES
    blocks = block_len.shape[0]
    Q = T - D - E
    cfg = (dp, grp, Y, Z, K, S, D, E, lines, piece)
    bf, f32 = jnp.bfloat16, jnp.float32
    dma = pltpu.SemaphoreType.DMA
    part = (half, lanes)
    scratch = [
        pltpu.SMEM(block_len.shape, jnp.int32),
        pltpu.SMEM(amax_history.shape, f32),
        pltpu.VMEM((dp, own_rows, lanes), bf),
        pltpu.VMEM((2, far, own_rows, lanes), bf),
        pltpu.VMEM((own_rows, lanes), bf),
        pltpu.VMEM((T - D,) + part, bf),
        pltpu.VMEM((Q, X) + part, bf),
        pltpu.VMEM((D, grp, sub, lanes), bf),
        pltpu.VMEM((E, CORES, X) + part, bf),
        pltpu.VMEM((Q,) + part, bf),
        pltpu.VMEM((Q,) + part, bf),
        pltpu.VMEM((own_rows, lanes), f32),
        pltpu.VMEM((own_rows, lanes), f32),
        pltpu.VMEM((own_rows, lanes), jnp.int32),
        pltpu.VMEM((blocks, 8, lanes), f32),
        pltpu.VMEM((1, lanes), f32),
        pltpu.VMEM((dp * grp, 1, lanes), f32),
        dma((2,)),
        dma((dp,)),
        dma((K,)), dma((2, far, K)), dma((2, T)),
        dma(()), dma((T - D,)),
        dma(()), dma((Q, X - 1)),
        dma(()), dma((Q,)),
        dma(()), dma((D, grp - 1)),
        dma(()), dma((E, grp - 1)),
        dma(()), dma(()),
    ]
    hbm = pl.BlockSpec(memory_space=pltpu.HBM)
    vmem = pl.BlockSpec(memory_space=pltpu.VMEM)
    anywhere = pl.BlockSpec(memory_space=pl.ANY)
    pinned = [
        pltpu.with_memory_space_constraint(a, pltpu.HBM)
        for a in (block_len, amax_history, gradients.reshape((dp, own_rows, lanes)))
    ]
    shapes = (
        jax.ShapeDtypeStruct((own_rows, lanes), bf),
        jax.ShapeDtypeStruct((blocks,), bf),
    )
    mean, top = pl.pallas_call(
        functools.partial(kernel, cfg),
        out_shape=shapes,
        in_specs=[hbm, hbm, hbm],
        out_specs=(vmem, vmem),
        scratch_shapes=scratch,
        compiler_params=pltpu.CompilerParams(
            collective_id=0, has_side_effects=True, vmem_limit_bytes=24 << 20
        ),
    )(*pinned)
    return pl.pallas_call(
        put_out,
        out_shape=shapes,
        in_specs=[anywhere, anywhere],
        out_specs=(hbm, hbm),
        scratch_shapes=[dma((2,))],
        compiler_params=pltpu.CompilerParams(vmem_limit_bytes=24 << 20),
    )(mean, top)


def solution(mesh):
    placed = (P("grp", "dp", None, None), P(), P())
    return jax.shard_map(
        body, mesh=mesh, in_specs=placed, out_specs=(P("dp", None), P()), check_vma=False
    )
```
